32 devices in a mesh: tower: 2 (over core), tp: 4 (over z), grp: 4 (over y, x).
Axes of the slice: x: 2, y: 2, z: 4, core: 2. Of those that a mesh axis runs over, the one named last changes fastest.
Arguments:
- tokens: bfloat16 [3072, 8192], P('grp', 'tp'), may hold values from -700 to 700
- modality: int32 [3072], P('grp'), may hold values from 0 to 1, as said below
- doc_ids: int32 [3072], P('grp'), may hold values from 0 to 15, as said below
- owner_ids: int32 [3072], P('grp'), may hold values from 0 to 3, as said below
- norm_gain: float32 [2, 8192], P('tower'), may hold values from 0.5 to 1.5
- query_weight: bfloat16 [2, 8192, 4096], P('tower', 'grp', 'tp'), may hold values from -0.125 to 0.125
- pair_weight: bfloat16 [2, 8192, 1024], P('tower', 'grp'), may hold values from -0.125 to 0.125
Outputs:
- attended: bfloat16 [2, 3072, 4096], P('tower', 'grp', 'tp')
The draws below stay inside these ranges and needn't reach their ends.
Inputs may be any that keep to these rules, and one draw needn't show every extreme that they name: Every group of 768 tokens holds exactly 384 tokens of each modality. `owner_ids`: within every group each owner is named by exactly 192 tokens, and by at most 192 tokens of one modality. `doc_ids`: all tokens of one document have the same owner.
All inputs are finite; a program needn't handle non-finite values.
Results may differ from the reference program's by a relative error of at most 0.0084.
Values may be sent and summed in bfloat16 or wider, within the bound.
A program may use at most 128 MiB of HBM per device.

```python
import math
import jax
import jax.numpy as jnp
from jax import lax

D = 8192
HD = 128
HEADS = 32
KV_HEADS = 4
TOK = 768
GROUPS = 4
SLOT = 192
TOKENS = 3072


WEIGHT_EDGE = 0.125


def layout(key):
    base_key = jax.random.fold_in(key, 1234)
    perm_key, run_key, star_key, cut_key = jax.random.split(base_key, 4)
    permuted = jax.vmap(lambda subkey: jax.random.permutation(subkey, TOK))(jax.random.split(perm_key, GROUPS)).astype(jnp.int32)
    owner_table = permuted // SLOT
    position = jnp.arange(TOK, dtype=jnp.int32)
    sorted_order = jnp.argsort(owner_table * TOK + position[None, :], axis=1).astype(jnp.int32)
    placed = jnp.argsort(sorted_order, axis=1).astype(jnp.int32)
    within = placed % SLOT
    first_half = jax.random.randint(run_key, (GROUPS, GROUPS // 2), 0, SLOT + 1)
    star_owner = jax.random.randint(star_key, (), 0, GROUPS)
    forced = jnp.where(star_owner % 2 == 0, SLOT, 0)
    first_half = jnp.where(jnp.arange(GROUPS // 2)[None, :] == star_owner // 2, forced, first_half)
    image_run = jnp.stack([first_half, SLOT - first_half], axis=2).reshape(GROUPS, GROUPS)
    run_here = jnp.take_along_axis(image_run, owner_table, axis=1)
    modality_table = (within < run_here).astype(jnp.int32)
    cut_flags = (jax.random.randint(cut_key, (GROUPS, GROUPS), 0, 4) == 0).astype(jnp.int32)
    cut_flags = cut_flags.at[GROUPS - 1, :].set(1)
    cut_flags = cut_flags.at[:, 0].set(0)
    segment = jnp.cumsum(cut_flags, axis=1)
    doc_table = owner_table * GROUPS + jnp.take_along_axis(segment.T, owner_table, axis=1)
    return (modality_table.reshape(-1), doc_table.reshape(-1).astype(jnp.int32), owner_table.reshape(-1))


def column_scale(key):
    return jnp.exp(jax.random.uniform(jax.random.fold_in(key, 77), (D,), jnp.float32, 0.0, math.log(10.0)))


def draw_modality(key, part):
    return layout(key)[0]


def draw_doc_ids(key, part):
    return layout(key)[1]


def draw_owner_ids(key, part):
    return layout(key)[2]


def draw_tokens(key, part):
    row_key, noise_key = jax.random.split(jax.random.fold_in(key, 11), 2)
    columns = column_scale(key)
    row_scales = jnp.exp(jax.random.uniform(row_key, (TOKENS, 1), jnp.float32, 0.0, math.log(10.0)))
    base_draw = jax.random.normal(noise_key, (TOKENS, D), jnp.float32)
    drawn = base_draw * row_scales * columns[None, :]
    return jnp.clip(drawn, -700.0, 700.0).astype(jnp.bfloat16)


def draw_query_weight(key, part):
    drawn = jax.random.normal(jax.random.fold_in(key, 21), (2, D, HEADS * HD), jnp.float32) / math.sqrt(D)
    return jnp.clip(drawn, -WEIGHT_EDGE, WEIGHT_EDGE).astype(jnp.bfloat16)


def draw_pair_weight(key, part):
    drawn = jax.random.normal(jax.random.fold_in(key, 31), (2, D, KV_HEADS, 2, HD), jnp.float32) / math.sqrt(D)
    return jnp.clip(drawn, -WEIGHT_EDGE, WEIGHT_EDGE).reshape(2, D, KV_HEADS * 2 * HD).astype(jnp.bfloat16)


def setup_inputs(seed: int = 0) -> dict:
    seeds = jax.random.split(jax.random.key(seed), 8)
    return {
        "tokens": draw_tokens(jax.random.fold_in(seeds[7], 71), 0),
        "modality": draw_modality(jax.random.fold_in(seeds[7], 71), 0),
        "doc_ids": draw_doc_ids(jax.random.fold_in(seeds[7], 71), 0),
        "owner_ids": draw_owner_ids(jax.random.fold_in(seeds[7], 71), 0),
        "norm_gain": jnp.clip(1.0 + 0.1 * jax.random.normal(seeds[4], (2, D), jnp.float32), 0.5, 1.5),
        "query_weight": draw_query_weight(jax.random.fold_in(seeds[7], 71), 0),
        "pair_weight": draw_pair_weight(jax.random.fold_in(seeds[7], 71), 0),
    }


EPS = 1e-05
MASKED = -1e+30

def normalize(rows, gain_row):
    values = rows.astype(jnp.float32)
    inverse_rms = lax.rsqrt(lax.optimization_barrier(jnp.mean(values * values, axis=1, keepdims=True)) + EPS)
    return (values * inverse_rms * gain_row[None, :]).astype(jnp.bfloat16)

def reference(tokens, modality, doc_ids, owner_ids, norm_gain, query_weight, pair_weight):
    query_all = jnp.zeros((TOKENS, HEADS * HD), jnp.bfloat16)
    pair_all = jnp.zeros((TOKENS, KV_HEADS * 2 * HD), jnp.bfloat16)
    for tower_index in range(2):
        picked = jnp.nonzero(modality == tower_index, size=TOKENS // 2)[0].astype(jnp.int32)
        normed = normalize(tokens[picked], norm_gain[tower_index])
        query_rows = jnp.dot(normed, query_weight[tower_index], preferred_element_type=jnp.float32).astype(jnp.bfloat16)
        pair_rows = jnp.dot(normed, pair_weight[tower_index], preferred_element_type=jnp.float32).astype(jnp.bfloat16)
        query_all = query_all.at[picked].set(query_rows)
        pair_all = pair_all.at[picked].set(pair_rows)
    sharing = HEADS // KV_HEADS
    scale_factor = 1.0 / math.sqrt(HD)

    def attend(owner_index):
        members = jnp.nonzero(owner_ids == owner_index, size=TOK)[0].astype(jnp.int32)
        queries = query_all[members].astype(jnp.float32).reshape(TOK, KV_HEADS, sharing, HD)
        pair_data = pair_all[members].astype(jnp.float32).reshape(TOK, KV_HEADS, 2, HD)
        doc_rows = doc_ids[members]
        images = modality[members] == 1
        allowed = (doc_rows[:, None] == doc_rows[None, :]) & ((members[None, :] <= members[:, None]) | images[:, None] & images[None, :])
        scores = jnp.einsum('qjgd,kjd->jgqk', queries, pair_data[:, :, 0]) * scale_factor
        scores = jnp.where(allowed[None, None], scores, MASKED)
        row_max = lax.optimization_barrier(jnp.max(scores, axis=3, keepdims=True))
        powered = jnp.exp(scores - row_max)
        weights = (powered / lax.optimization_barrier(jnp.sum(powered, axis=3, keepdims=True))).astype(jnp.bfloat16)
        mixed_rows = jnp.einsum('jgqk,kjd->qjgd', weights.astype(jnp.float32), pair_data[:, :, 1])
        return (mixed_rows.astype(jnp.bfloat16).reshape(TOK, HEADS * HD), members)
    outputs, member_lists = lax.map(attend, jnp.arange(GROUPS, dtype=jnp.int32))
    attention = jnp.zeros((TOKENS, HEADS * HD), jnp.bfloat16).at[member_lists.reshape(-1)].set(outputs.reshape(TOKENS, HEADS * HD))
    towers = jnp.arange(2, dtype=jnp.int32)
    return jnp.where(modality[None, :, None] == towers[:, None, None], attention[None], jnp.zeros((), jnp.bfloat16))
```

```python
import math

import jax
import jax.numpy as jnp
from jax import lax
from jax.sharding import PartitionSpec as P

HD = 128
EPS = 1e-05
MASKED = -1e30


def swap_tower(value):
    return lax.ppermute(value, "tower", [(0, 1), (1, 0)])


def pick(onehot, rows):
    return jnp.dot(onehot.astype(jnp.bfloat16), rows, preferred_element_type=jnp.float32).astype(
        jnp.bfloat16
    )


def move_tokens(chosen):
    gathered = lax.all_gather(chosen, "tp", axis=0, tiled=False)
    return lax.all_to_all(gathered, "grp", split_axis=0, concat_axis=0, tiled=True)


def to_owner(partial):
    return lax.all_to_all(partial, "grp", split_axis=0, concat_axis=0, tiled=True)


def local(tokens, modality, doc_ids, owner_ids, norm_gain, query_weight, pair_weight):
    groups = lax.axis_size("grp")
    tp_count = lax.axis_size("tp")
    tower = lax.axis_index("tower")
    group = lax.axis_index("grp")
    tp_rank = lax.axis_index("tp")
    tok, width = tokens.shape
    half = tok // 2
    slot_count = tok // groups
    head_cols = query_weight.shape[2]
    pair_heads = pair_weight.shape[2] // (2 * HD)
    own_head = tp_rank // (tp_count // pair_heads)
    features = width * tp_count
    bf16, f32, i32 = jnp.bfloat16, jnp.float32, jnp.int32

    values = tokens.astype(f32)
    code = (doc_ids * groups + owner_ids) * 2 + modality
    facts = jnp.stack([code.astype(f32), jnp.sum(values * values, axis=1)])
    facts = lax.all_gather(facts, ("grp", "tp"), axis=0, tiled=False)
    facts = facts.reshape(groups, tp_count, 2, tok)
    codes = facts[:, 0, 0, :].astype(i32)
    mods = codes % 2
    owners = (codes // 2) % groups
    squares = jnp.sum(lax.dynamic_index_in_dim(facts, group, 0, False)[:, 1, :], axis=0)
    inverse_rms = lax.rsqrt(squares / features + EPS)

    where_i = jnp.arange(tok, dtype=i32)
    before = (where_i[None, :] < where_i[:, None])[None]
    owner_rank = jnp.sum(((owners[:, None, :] == owners[:, :, None]) & before).astype(i32), axis=2)
    mod_rank = jnp.sum(((mods[:, None, :] == mods[:, :, None]) & before).astype(i32), axis=2)
    slots = owners * slot_count + owner_rank
    packed = mods * half + mod_rank
    at_slot = slots[:, None, :] == where_i[None, :, None]
    packed_of_slot = jnp.sum(jnp.where(at_slot, packed[:, None, :], 0), axis=2)

    slots_here = lax.dynamic_index_in_dim(slots, group, 0, False)
    packed_here = lax.dynamic_index_in_dim(packed, group, 0, False)

    gain = lax.dynamic_slice_in_dim(norm_gain[0], tp_rank * width, width, 0)
    normed = (values * inverse_rms[:, None] * gain[None, :]).astype(bf16)
    choose = packed_here[None, :] == (tower * half + jnp.arange(half, dtype=i32))[:, None]
    chosen = pick(choose, normed)
    arrived = move_tokens(chosen).reshape(groups * half, width)

    pair_part = lax.dynamic_slice_in_dim(pair_weight[0], own_head * 2 * HD, 2 * HD, 1)
    half_cols = head_cols // 2
    query_part = jnp.dot(arrived, query_weight[0], preferred_element_type=f32).astype(bf16)
    pair_part = jnp.dot(arrived, pair_part, preferred_element_type=f32).astype(bf16)
    query_keep = lax.dynamic_slice_in_dim(query_part, tower * half_cols, half_cols, 1)
    query_give = lax.dynamic_slice_in_dim(query_part, (1 - tower) * half_cols, half_cols, 1)
    keep = jnp.concatenate([query_keep, pair_part], axis=1)
    got = swap_tower(jnp.concatenate([query_give, pair_part], axis=1))
    cols = half_cols + 2 * HD
    keep = keep.reshape(groups, half, cols)
    got = got.reshape(groups, half, cols)
    own_first = jnp.concatenate([keep, got], axis=1)
    position = packed_of_slot - tower * half
    position = jnp.where(position < 0, position + tok, position)
    expand = (position[:, :, None] == where_i[None, None, :]).astype(bf16)
    slotted = jnp.einsum("gsp,gpc->gsc", expand, own_first, preferred_element_type=f32).astype(bf16)
    by_owner = slotted.reshape(groups, groups, slot_count, cols).transpose(1, 0, 2, 3)
    parts = to_owner(by_owner.reshape(groups, tok, cols))
    rows = jnp.sum(parts.astype(f32), axis=0).astype(bf16)

    mine = group * slot_count + jnp.arange(slot_count, dtype=i32)
    at_mine = slots[:, None, :] == mine[None, :, None]
    code_mine = jnp.sum(jnp.where(at_mine, codes[:, None, :], 0), axis=2).reshape(tok)
    place_mine = jnp.sum(jnp.where(at_mine, where_i[None, None, :], 0), axis=2)
    place_mine = (place_mine + tok * jnp.arange(groups, dtype=i32)[:, None]).reshape(tok)
    image = code_mine % 2 == 1
    doc = code_mine // (2 * groups)
    allowed = (doc[:, None] == doc[None, :]) & (
        (place_mine[None, :] <= place_mine[:, None]) | (image[:, None] & image[None, :])
    )
    heads = half_cols // HD
    queries = rows[:, :half_cols].reshape(tok, heads, HD)
    keys = rows[:, half_cols : half_cols + HD]
    vals = rows[:, half_cols + HD :]
    scores = jnp.einsum("qhd,kd->hqk", queries, keys, preferred_element_type=f32) * (
        1.0 / math.sqrt(HD)
    )
    scores = jnp.where(allowed[None], scores, MASKED)
    powered = jnp.exp(scores - jnp.max(scores, axis=2, keepdims=True))
    weights = (powered / jnp.sum(powered, axis=2, keepdims=True)).astype(bf16)
    mixed = jnp.einsum("hqk,kd->qhd", weights, vals, preferred_element_type=f32)
    mixed = mixed.astype(bf16).reshape(tok, half_cols)

    returned = lax.all_to_all(mixed, "grp", split_axis=0, concat_axis=0, tiled=True)
    other = swap_tower(returned)
    left = jnp.where(tower == 0, returned, other)
    right = jnp.where(tower == 0, other, returned)
    in_tower = modality == tower
    place = (slots_here[:, None] == where_i[None, :]) & in_tower[:, None]
    result = pick(place, jnp.concatenate([left, right], axis=1))
    return result[None]


def solution(mesh):
    in_specs = (
        P("grp", "tp"),
        P("grp"),
        P("grp"),
        P("grp"),
        P("tower", None),
        P("tower", "grp", "tp"),
        P("tower", "grp", None),
    )
    out_specs = P("tower", "grp", "tp")
    return jax.shard_map(local, mesh=mesh, in_specs=in_specs, out_specs=out_specs, check_vma=False)
```

```python
import functools
import math

import jax
import jax.numpy as jnp
from jax import lax
from jax.experimental import pallas as pl
from jax.experimental.pallas import tpu as pltpu
from jax.sharding import PartitionSpec as P

HD = 128
EPS = 1e-05
MASKED = -1e30


def swap_tower(value):
    return lax.ppermute(value, "tower", [(0, 1), (1, 0)])


def pick(onehot, rows):
    return jnp.dot(onehot.astype(jnp.bfloat16), rows, preferred_element_type=jnp.float32).astype(
        jnp.bfloat16
    )


MESH = pl.DeviceIdType.MESH


def greet(devices):
    barrier = pltpu.get_barrier_semaphore()
    for present, device in devices:

        @pl.when(present)
        def _(device=device):
            pl.semaphore_signal(barrier, inc=1, device_id=device, device_id_type=MESH)

    pl.semaphore_wait(barrier, sum(jnp.asarray(present, jnp.int32) for present, _ in devices))


def others(axis, count):
    me = lax.axis_index(axis)
    return [(True, {axis: lax.rem(me + k, count)}) for k in range(1, count)]


def facts_kernel(groups, tp_count, facts, by_group, by_block, send_sem, group_sem, block_sem):
    group, block = lax.axis_index("grp"), lax.axis_index("tp")
    greet(others("grp", groups) + others("tp", tp_count))
    sent = []
    for k in range(1, groups):
        sent.append(
            pltpu.make_async_remote_copy(
                src_ref=facts,
                dst_ref=by_group.at[group],
                send_sem=send_sem.at[k - 1],
                recv_sem=group_sem.at[group],
                device_id={"grp": lax.rem(group + k, groups)},
                device_id_type=MESH,
            )
        )
    for k in range(1, tp_count):
        sent.append(
            pltpu.make_async_remote_copy(
                src_ref=facts,
                dst_ref=by_block.at[block],
                send_sem=send_sem.at[groups + k - 2],
                recv_sem=block_sem.at[block],
                device_id={"tp": lax.rem(block + k, tp_count)},
                device_id_type=MESH,
            )
        )
    for copy in sent:
        copy.start()
    by_group[group] = facts[...]
    by_block[block] = facts[...]
    for k in range(1, groups):
        source = lax.rem(group + k, groups)
        pltpu.make_async_copy(facts, by_group.at[source], group_sem.at[source]).wait()
    for k in range(1, tp_count):
        source = lax.rem(block + k, tp_count)
        pltpu.make_async_copy(facts, by_block.at[source], block_sem.at[source]).wait()
    for copy in sent:
        copy.wait_send()


def share_facts(facts, groups, tp_count):
    vmem = pl.BlockSpec(memory_space=pltpu.VMEM)
    return pl.pallas_call(
        functools.partial(facts_kernel, groups, tp_count),
        out_shape=[
            jax.ShapeDtypeStruct((groups,) + facts.shape, facts.dtype),
            jax.ShapeDtypeStruct((tp_count,) + facts.shape, facts.dtype),
        ],
        in_specs=[vmem],
        out_specs=[vmem, vmem],
        scratch_shapes=[
            pltpu.SemaphoreType.DMA((groups + tp_count - 2,)),
            pltpu.SemaphoreType.DMA((groups,)),
            pltpu.SemaphoreType.DMA((tp_count,)),
        ],
        compiler_params=pltpu.CompilerParams(collective_id=1, has_side_effects=True),
        name="share_facts",
    )(facts)


def tokens_kernel(
    groups, count, chunks, chosen, out, held, own_sem, line_send, line_recv, cross_send, cross_recv
):
    group, me = lax.axis_index("grp"), lax.axis_index("tp")
    rows = chosen.shape[0] // chunks
    has_left, has_right = me > 0, me < count - 1
    left, right = jnp.maximum(me - 1, 0), jnp.minimum(me + 1, count - 1)
    greet([(has_left, {"tp": left}), (has_right, {"tp": right})] + others("grp", groups))

    def part(chunk):
        return pl.ds(pl.multiple_of(chunk * rows, rows), rows)

    def hop(source, chunk, way, own):
        src = chosen if own else held.at[source]
        return pltpu.make_async_remote_copy(
            src_ref=src.at[part(chunk)],
            dst_ref=held.at[source, part(chunk)],
            send_sem=line_send.at[way, source, chunk],
            recv_sem=line_recv.at[source, chunk],
            device_id={"tp": left if way == 0 else right},
            device_id_type=MESH,
        )

    def cross(source, chunk, own):
        src = chosen if own else held.at[source]
        return pltpu.make_async_remote_copy(
            src_ref=src.at[part(chunk)],
            dst_ref=out.at[group, part(chunk)],
            send_sem=cross_send.at[source, chunk],
            recv_sem=cross_recv.at[group, chunk],
            device_id={"grp": source},
            device_id_type=MESH,
        )

    def keep(source, chunk, own):
        src = chosen if own else held.at[source]
        return pltpu.make_async_copy(
            src.at[part(chunk)], out.at[group, part(chunk)], own_sem.at[chunk]
        )

    def pass_on(source, chunk, own):
        @pl.when(source == group)
        def _():
            keep(source, chunk, own).start()

        @pl.when(source != group)
        def _():
            cross(source, chunk, own).start()

    def start_own(chunk):
        @pl.when(has_left)
        def _():
            hop(me, chunk, 0, True).start()

        @pl.when(has_right)
        def _():
            hop(me, chunk, 1, True).start()

        pass_on(me, chunk, True)

    def arrive(source, chunk, way, more):
        hop(source, chunk, way, False).wait_recv()

        @pl.when(more)
        def _():
            hop(source, chunk, way, False).start()

        pass_on(source, chunk, False)

    start_own(0)

    @pl.loop(0, chunks)
    def _(chunk):
        @pl.when(chunk + 1 < chunks)
        def _():
            start_own(chunk + 1)

        for k in range(1, count):

            @pl.when(me + k < count)
            def _():
                arrive(me + k, chunk, 0, has_left)

            @pl.when(me - k >= 0)
            def _():
                arrive(me - k, chunk, 1, has_right)

    @pl.loop(0, chunks)
    def _(chunk):
        for k in range(1, groups):
            source = lax.rem(group + k, groups)
            pltpu.make_async_copy(
                chosen.at[part(chunk)], out.at[source, part(chunk)], cross_recv.at[source, chunk]
            ).wait()
        keep(group, chunk, False).wait()
        for source in range(count):

            @pl.when(source != group)
            def _():
                cross(source, chunk, False).wait_send()

            @pl.when((source >= me) & has_left)
            def _():
                hop(source, chunk, 0, False).wait_send()

            @pl.when((source <= me) & has_right)
            def _():
                hop(source, chunk, 1, False).wait_send()


def move_tokens(chosen, groups, tp_count):
    half, width = chosen.shape
    chunks = max(1, 24 // tp_count)
    while half % chunks or (half // chunks) % 16:
        chunks -= 1
    vmem = pl.BlockSpec(memory_space=pltpu.VMEM)
    return pl.pallas_call(
        functools.partial(tokens_kernel, groups, tp_count, chunks),
        out_shape=jax.ShapeDtypeStruct((groups, half, width), chosen.dtype),
        in_specs=[vmem],
        out_specs=vmem,
        scratch_shapes=[
            pltpu.VMEM((tp_count, half, width), chosen.dtype),
            pltpu.SemaphoreType.DMA((chunks,)),
            pltpu.SemaphoreType.DMA((2, tp_count, chunks)),
            pltpu.SemaphoreType.DMA((tp_count, chunks)),
            pltpu.SemaphoreType.DMA((tp_count, chunks)),
            pltpu.SemaphoreType.DMA((groups, chunks)),
        ],
        compiler_params=pltpu.CompilerParams(
            collective_id=2, has_side_effects=True, vmem_limit_bytes=40 * 2**20
        ),
        name="move_tokens",
    )(chosen)


def to_owner(partial):
    return lax.all_to_all(partial, "grp", split_axis=0, concat_axis=0, tiled=True)


def local(tokens, modality, doc_ids, owner_ids, norm_gain, query_weight, pair_weight):
    groups = lax.axis_size("grp")
    tp_count = lax.axis_size("tp")
    tower = lax.axis_index("tower")
    group = lax.axis_index("grp")
    tp_rank = lax.axis_index("tp")
    tok, width = tokens.shape
    half = tok // 2
    slot_count = tok // groups
    head_cols = query_weight.shape[2]
    pair_heads = pair_weight.shape[2] // (2 * HD)
    own_head = tp_rank // (tp_count // pair_heads)
    features = width * tp_count
    bf16, f32, i32 = jnp.bfloat16, jnp.float32, jnp.int32

    values = tokens.astype(f32)
    code = (doc_ids * groups + owner_ids) * 2 + modality
    squares = jnp.sum(values * values, axis=1)
    row = jnp.arange(8, dtype=i32)[:, None]
    facts = jnp.where(row == 0, code.astype(f32)[None, :], jnp.where(row == 1, squares[None, :], 0.0))
    by_group, by_block = share_facts(facts, groups, tp_count)
    codes = by_group[:, 0, :].astype(i32)
    mods = codes % 2
    owners = (codes // 2) % groups
    squares = jnp.sum(by_block[:, 1, :], axis=0)
    inverse_rms = lax.rsqrt(squares / features + EPS)

    where_i = jnp.arange(tok, dtype=i32)
    before = (where_i[None, :] < where_i[:, None])[None]
    owner_rank = jnp.sum(((owners[:, None, :] == owners[:, :, None]) & before).astype(i32), axis=2)
    mod_rank = jnp.sum(((mods[:, None, :] == mods[:, :, None]) & before).astype(i32), axis=2)
    slots = owners * slot_count + owner_rank
    packed = mods * half + mod_rank
    at_slot = slots[:, None, :] == where_i[None, :, None]
    packed_of_slot = jnp.sum(jnp.where(at_slot, packed[:, None, :], 0), axis=2)

    slots_here = lax.dynamic_index_in_dim(slots, group, 0, False)
    packed_here = lax.dynamic_index_in_dim(packed, group, 0, False)

    gain = lax.dynamic_slice_in_dim(norm_gain[0], tp_rank * width, width, 0)
    normed = (values * inverse_rms[:, None] * gain[None, :]).astype(bf16)
    choose = packed_here[None, :] == (tower * half + jnp.arange(half, dtype=i32))[:, None]
    chosen = pick(choose, normed)
    arrived = move_tokens(chosen, groups, tp_count).reshape(groups * half, width)

    pair_part = lax.dynamic_slice_in_dim(pair_weight[0], own_head * 2 * HD, 2 * HD, 1)
    half_cols = head_cols // 2
    query_part = jnp.dot(arrived, query_weight[0], preferred_element_type=f32).astype(bf16)
    pair_part = jnp.dot(arrived, pair_part, preferred_element_type=f32).astype(bf16)
    query_keep = lax.dynamic_slice_in_dim(query_part, tower * half_cols, half_cols, 1)
    query_give = lax.dynamic_slice_in_dim(query_part, (1 - tower) * half_cols, half_cols, 1)
    keep = jnp.concatenate([query_keep, pair_part], axis=1)
    got = swap_tower(jnp.concatenate([query_give, pair_part], axis=1))
    cols = half_cols + 2 * HD
    keep = keep.reshape(groups, half, cols)
    got = got.reshape(groups, half, cols)
    own_first = jnp.concatenate([keep, got], axis=1)
    position = packed_of_slot - tower * half
    position = jnp.where(position < 0, position + tok, position)
    expand = (position[:, :, None] == where_i[None, None, :]).astype(bf16)
    slotted = jnp.einsum("gsp,gpc->gsc", expand, own_first, preferred_element_type=f32).astype(bf16)
    by_owner = slotted.reshape(groups, groups, slot_count, cols).transpose(1, 0, 2, 3)
    parts = to_owner(by_owner.reshape(groups, tok, cols))
    rows = jnp.sum(parts.astype(f32), axis=0).astype(bf16)

    mine = group * slot_count + jnp.arange(slot_count, dtype=i32)
    at_mine = slots[:, None, :] == mine[None, :, None]
    code_mine = jnp.sum(jnp.where(at_mine, codes[:, None, :], 0), axis=2).reshape(tok)
    place_mine = jnp.sum(jnp.where(at_mine, where_i[None, None, :], 0), axis=2)
    place_mine = (place_mine + tok * jnp.arange(groups, dtype=i32)[:, None]).reshape(tok)
    image = code_mine % 2 == 1
    doc = code_mine // (2 * groups)
    allowed = (doc[:, None] == doc[None, :]) & (
        (place_mine[None, :] <= place_mine[:, None]) | (image[:, None] & image[None, :])
    )
    heads = half_cols // HD
    queries = rows[:, :half_cols].reshape(tok, heads, HD)
    keys = rows[:, half_cols : half_cols + HD]
    vals = rows[:, half_cols + HD :]
    scores = jnp.einsum("qhd,kd->hqk", queries, keys, preferred_element_type=f32) * (
        1.0 / math.sqrt(HD)
    )
    scores = jnp.where(allowed[None], scores, MASKED)
    powered = jnp.exp(scores - jnp.max(scores, axis=2, keepdims=True))
    weights = (powered / jnp.sum(powered, axis=2, keepdims=True)).astype(bf16)
    mixed = jnp.einsum("hqk,kd->qhd", weights, vals, preferred_element_type=f32)
    mixed = mixed.astype(bf16).reshape(tok, half_cols)

    returned = lax.all_to_all(mixed, "grp", split_axis=0, concat_axis=0, tiled=True)
    other = swap_tower(returned)
    left = jnp.where(tower == 0, returned, other)
    right = jnp.where(tower == 0, other, returned)
    in_tower = modality == tower
    place = (slots_here[:, None] == where_i[None, :]) & in_tower[:, None]
    result = pick(place, jnp.concatenate([left, right], axis=1))
    return result[None]


def solution(mesh):
    in_specs = (
        P("grp", "tp"),
        P("grp"),
        P("grp"),
        P("grp"),
        P("tower", None),
        P("tower", "grp", "tp"),
        P("tower", "grp", None),
    )
    out_specs = P("tower", "grp", "tp")
    return jax.shard_map(local, mesh=mesh, in_specs=in_specs, out_specs=out_specs, check_vma=False)
```

```python
import functools
import math

import jax
import jax.numpy as jnp
from jax import lax
from jax.experimental import pallas as pl
from jax.experimental.pallas import tpu as pltpu
from jax.sharding import PartitionSpec as P

HD = 128
EPS = 1e-05
MASKED = -1e30


def swap_tower(value):
    return lax.ppermute(value, "tower", [(0, 1), (1, 0)])


def pick(onehot, rows):
    return jnp.dot(onehot.astype(jnp.bfloat16), rows, preferred_element_type=jnp.float32).astype(
        jnp.bfloat16
    )


MESH = pl.DeviceIdType.MESH


def greet(devices):
    barrier = pltpu.get_barrier_semaphore()
    for present, device in devices:

        @pl.when(present)
        def _(device=device):
            pl.semaphore_signal(barrier, inc=1, device_id=device, device_id_type=MESH)

    pl.semaphore_wait(barrier, sum(jnp.asarray(present, jnp.int32) for present, _ in devices))


def others(axis, count):
    me = lax.axis_index(axis)
    return [(True, {axis: lax.rem(me + k, count)}) for k in range(1, count)]


def facts_kernel(groups, tp_count, facts, by_group, by_block, send_sem, group_sem, block_sem):
    group, block = lax.axis_index("grp"), lax.axis_index("tp")
    greet(others("grp", groups) + others("tp", tp_count))
    sent = []
    for k in range(1, groups):
        sent.append(
            pltpu.make_async_remote_copy(
                src_ref=facts,
                dst_ref=by_group.at[group],
                send_sem=send_sem.at[k - 1],
                recv_sem=group_sem.at[group],
                device_id={"grp": lax.rem(group + k, groups)},
                device_id_type=MESH,
            )
        )
    for k in range(1, tp_count):
        sent.append(
            pltpu.make_async_remote_copy(
                src_ref=facts,
                dst_ref=by_block.at[block],
                send_sem=send_sem.at[groups + k - 2],
                recv_sem=block_sem.at[block],
                device_id={"tp": lax.rem(block + k, tp_count)},
                device_id_type=MESH,
            )
        )
    for copy in sent:
        copy.start()
    by_group[group] = facts[...]
    by_block[block] = facts[...]
    for k in range(1, groups):
        source = lax.rem(group + k, groups)
        pltpu.make_async_copy(facts, by_group.at[source], group_sem.at[source]).wait()
    for k in range(1, tp_count):
        source = lax.rem(block + k, tp_count)
        pltpu.make_async_copy(facts, by_block.at[source], block_sem.at[source]).wait()
    for copy in sent:
        copy.wait_send()


def share_facts(facts, groups, tp_count):
    vmem = pl.BlockSpec(memory_space=pltpu.VMEM)
    return pl.pallas_call(
        functools.partial(facts_kernel, groups, tp_count),
        out_shape=[
            jax.ShapeDtypeStruct((groups,) + facts.shape, facts.dtype),
            jax.ShapeDtypeStruct((tp_count,) + facts.shape, facts.dtype),
        ],
        in_specs=[vmem],
        out_specs=[vmem, vmem],
        scratch_shapes=[
            pltpu.SemaphoreType.DMA((groups + tp_count - 2,)),
            pltpu.SemaphoreType.DMA((groups,)),
            pltpu.SemaphoreType.DMA((tp_count,)),
        ],
        compiler_params=pltpu.CompilerParams(collective_id=1, has_side_effects=True),
        name="share_facts",
    )(facts)


def tokens_kernel(
    groups, count, chunks, chosen, out, held, own_sem, line_send, line_recv, cross_send, cross_recv
):
    group, me = lax.axis_index("grp"), lax.axis_index("tp")
    rows = chosen.shape[0] // chunks
    has_left, has_right = me > 0, me < count - 1
    left, right = jnp.maximum(me - 1, 0), jnp.minimum(me + 1, count - 1)
    greet([(has_left, {"tp": left}), (has_right, {"tp": right})] + others("grp", groups))

    def part(chunk):
        return pl.ds(pl.multiple_of(chunk * rows, rows), rows)

    def hop(source, chunk, way, own):
        src = chosen if own else held.at[source]
        return pltpu.make_async_remote_copy(
            src_ref=src.at[part(chunk)],
            dst_ref=held.at[source, part(chunk)],
            send_sem=line_send.at[way, source, chunk],
            recv_sem=line_recv.at[source, chunk],
            device_id={"tp": left if way == 0 else right},
            device_id_type=MESH,
        )

    def cross(source, chunk, own):
        src = chosen if own else held.at[source]
        return pltpu.make_async_remote_copy(
            src_ref=src.at[part(chunk)],
            dst_ref=out.at[group, part(chunk)],
            send_sem=cross_send.at[source, chunk],
            recv_sem=cross_recv.at[group, chunk],
            device_id={"grp": source},
            device_id_type=MESH,
        )

    def keep(source, chunk, own):
        src = chosen if own else held.at[source]
        return pltpu.make_async_copy(
            src.at[part(chunk)], out.at[group, part(chunk)], own_sem.at[chunk]
        )

    def pass_on(source, chunk, own):
        @pl.when(source == group)
        def _():
            keep(source, chunk, own).start()

        @pl.when(source != group)
        def _():
            cross(source, chunk, own).start()

    def start_own(chunk):
        @pl.when(has_left)
        def _():
            hop(me, chunk, 0, True).start()

        @pl.when(has_right)
        def _():
            hop(me, chunk, 1, True).start()

        pass_on(me, chunk, True)

    def arrive(source, chunk, way, more):
        hop(source, chunk, way, False).wait_recv()

        @pl.when(more)
        def _():
            hop(source, chunk, way, False).start()

        pass_on(source, chunk, False)

    start_own(0)

    @pl.loop(0, chunks)
    def _(chunk):
        @pl.when(chunk + 1 < chunks)
        def _():
            start_own(chunk + 1)

        for k in range(1, count):

            @pl.when(me + k < count)
            def _():
                arrive(me + k, chunk, 0, has_left)

            @pl.when(me - k >= 0)
            def _():
                arrive(me - k, chunk, 1, has_right)

    @pl.loop(0, chunks)
    def _(chunk):
        for k in range(1, groups):
            source = lax.rem(group + k, groups)
            pltpu.make_async_copy(
                chosen.at[part(chunk)], out.at[source, part(chunk)], cross_recv.at[source, chunk]
            ).wait()
        keep(group, chunk, False).wait()
        for source in range(count):

            @pl.when(source != group)
            def _():
                cross(source, chunk, False).wait_send()

            @pl.when((source >= me) & has_left)
            def _():
                hop(source, chunk, 0, False).wait_send()

            @pl.when((source <= me) & has_right)
            def _():
                hop(source, chunk, 1, False).wait_send()


def move_tokens(chosen, groups, tp_count):
    half, width = chosen.shape
    chunks = max(1, 24 // tp_count)
    while half % chunks or (half // chunks) % 16:
        chunks -= 1
    vmem = pl.BlockSpec(memory_space=pltpu.VMEM)
    return pl.pallas_call(
        functools.partial(tokens_kernel, groups, tp_count, chunks),
        out_shape=jax.ShapeDtypeStruct((groups, half, width), chosen.dtype),
        in_specs=[vmem],
        out_specs=vmem,
        scratch_shapes=[
            pltpu.VMEM((tp_count, half, width), chosen.dtype),
            pltpu.SemaphoreType.DMA((chunks,)),
            pltpu.SemaphoreType.DMA((2, tp_count, chunks)),
            pltpu.SemaphoreType.DMA((tp_count, chunks)),
            pltpu.SemaphoreType.DMA((tp_count, chunks)),
            pltpu.SemaphoreType.DMA((groups, chunks)),
        ],
        compiler_params=pltpu.CompilerParams(
            collective_id=2, has_side_effects=True, vmem_limit_bytes=40 * 2**20
        ),
        name="move_tokens",
    )(chosen)


def to_owner(partial):
    return lax.all_to_all(partial, "grp", split_axis=0, concat_axis=0, tiled=True)


def local(tokens, modality, doc_ids, owner_ids, norm_gain, query_weight, pair_weight):
    groups = lax.axis_size("grp")
    tp_count = lax.axis_size("tp")
    tower = lax.axis_index("tower")
    group = lax.axis_index("grp")
    tp_rank = lax.axis_index("tp")
    tok, width = tokens.shape
    half = tok // 2
    slot_count = tok // groups
    head_cols = query_weight.shape[2]
    pair_heads = pair_weight.shape[2] // (2 * HD)
    own_head = tp_rank // (tp_count // pair_heads)
    features = width * tp_count
    bf16, f32, i32 = jnp.bfloat16, jnp.float32, jnp.int32

    values = tokens.astype(f32)
    code = (doc_ids * groups + owner_ids) * 2 + modality
    squares = jnp.sum(values * values, axis=1)
    row = jnp.arange(8, dtype=i32)[:, None]
    facts = jnp.where(row == 0, code.astype(f32)[None, :], jnp.where(row == 1, squares[None, :], 0.0))
    by_group, by_block = share_facts(facts, groups, tp_count)
    codes = by_group[:, 0, :].astype(i32)
    mods = codes % 2
    owners = (codes // 2) % groups
    squares = jnp.sum(by_block[:, 1, :], axis=0)
    inverse_rms = lax.rsqrt(squares / features + EPS)

    where_i = jnp.arange(tok, dtype=i32)
    before = (where_i[None, :] < where_i[:, None])[None]
    owner_rank = jnp.sum(((owners[:, None, :] == owners[:, :, None]) & before).astype(i32), axis=2)
    mod_rank = jnp.sum(((mods[:, None, :] == mods[:, :, None]) & before).astype(i32), axis=2)
    slots = owners * slot_count + owner_rank
    packed = mods * half + mod_rank
    at_slot = slots[:, None, :] == where_i[None, :, None]
    packed_of_slot = jnp.sum(jnp.where(at_slot, packed[:, None, :], 0), axis=2)

    slots_here = lax.dynamic_index_in_dim(slots, group, 0, False)
    packed_here = lax.dynamic_index_in_dim(packed, group, 0, False)

    gain = lax.dynamic_slice_in_dim(norm_gain[0], tp_rank * width, width, 0)
    normed = (values * inverse_rms[:, None] * gain[None, :]).astype(bf16)
    choose = packed_here[None, :] == (tower * half + jnp.arange(half, dtype=i32))[:, None]
    chosen = pick(choose, normed)
    arrived = move_tokens(chosen, groups, tp_count)

    pair_cut = lax.dynamic_slice_in_dim(pair_weight[0], own_head * 2 * HD, 2 * HD, 1)
    half_cols = head_cols // 2
    cols = half_cols + HD
    position = packed_of_slot - tower * half
    position = jnp.where(position < 0, position + tok, position)
    pieces = 2
    step = groups // pieces
    summed = []
    for piece in range(pieces):
        these = arrived[piece * step : (piece + 1) * step].reshape(step * half, width)
        query_part = jnp.dot(these, query_weight[0], preferred_element_type=f32).astype(bf16)
        pair_part = jnp.dot(these, pair_cut, preferred_element_type=f32).astype(bf16)

        def columns(core):
            return jnp.concatenate(
                [
                    lax.dynamic_slice_in_dim(query_part, core * half_cols, half_cols, 1),
                    lax.dynamic_slice_in_dim(pair_part, core * HD, HD, 1),
                ],
                axis=1,
            )

        got = swap_tower(columns(1 - tower))
        kept = columns(tower)
        slotted = []
        for k in range(step):
            onehot = (position[piece * step + k][:, None] == where_i[None, :]).astype(bf16)
            span = slice(k * half, (k + 1) * half)
            both = jnp.dot(onehot[:, :half], kept[span], preferred_element_type=f32)
            both += jnp.dot(onehot[:, half:], got[span], preferred_element_type=f32)
            slotted.append(both.astype(bf16).reshape(groups, slot_count, cols))
        parts = to_owner(jnp.concatenate(slotted, axis=1))
        summed.append(jnp.sum(parts.astype(f32), axis=0).astype(bf16))
    rows = jnp.concatenate(summed, axis=0)
    own_side = rows[:, half_cols:]
    far_side = swap_tower(own_side)
    keys = jnp.where(tower == 0, own_side, far_side)
    vals = jnp.where(tower == 0, far_side, own_side)

    mine = group * slot_count + jnp.arange(slot_count, dtype=i32)
    at_mine = slots[:, None, :] == mine[None, :, None]
    code_mine = jnp.sum(jnp.where(at_mine, codes[:, None, :], 0), axis=2).reshape(tok)
    place_mine = jnp.sum(jnp.where(at_mine, where_i[None, None, :], 0), axis=2)
    place_mine = (place_mine + tok * jnp.arange(groups, dtype=i32)[:, None]).reshape(tok)
    image = code_mine % 2 == 1
    doc = code_mine // (2 * groups)
    allowed = (doc[:, None] == doc[None, :]) & (
        (place_mine[None, :] <= place_mine[:, None]) | (image[:, None] & image[None, :])
    )
    heads = half_cols // HD
    queries = rows[:, :half_cols].reshape(tok, heads, HD)
    scores = jnp.einsum("qhd,kd->hqk", queries, keys, preferred_element_type=f32) * (
        1.0 / math.sqrt(HD)
    )
    scores = jnp.where(allowed[None], scores, MASKED)
    powered = jnp.exp(scores - jnp.max(scores, axis=2, keepdims=True))
    weights = (powered / jnp.sum(powered, axis=2, keepdims=True)).astype(bf16)
    mixed = jnp.einsum("hqk,kd->qhd", weights, vals, preferred_element_type=f32)
    mixed = mixed.astype(bf16).reshape(tok, half_cols)

    returned = lax.all_to_all(mixed, "grp", split_axis=0, concat_axis=0, tiled=True)
    other = swap_tower(returned)
    left = jnp.where(tower == 0, returned, other)
    right = jnp.where(tower == 0, other, returned)
    in_tower = modality == tower
    place = (slots_here[:, None] == where_i[None, :]) & in_tower[:, None]
    result = pick(place, jnp.concatenate([left, right], axis=1))
    return result[None]


def solution(mesh):
    in_specs = (
        P("grp", "tp"),
        P("grp"),
        P("grp"),
        P("grp"),
        P("tower", None),
        P("tower", "grp", "tp"),
        P("tower", "grp", None),
    )
    out_specs = P("tower", "grp", "tp")
    return jax.shard_map(local, mesh=mesh, in_specs=in_specs, out_specs=out_specs, check_vma=False)
```
